32 devices in a mesh: head: 4 (over y, core), seq: 8 (over z, x).
Axes of the slice: x: 2, y: 2, z: 4, core: 2. Of those that a mesh axis runs over, the one named last changes fastest.
Arguments:
- keys: bfloat16 [12288, 2560], P('seq', 'head'), may hold values from -6 to 6
- values: bfloat16 [12288, 2560], P('seq', 'head'), may hold values from -6 to 6
- queries: bfloat16 [12288, 2560], P('seq', 'head'), may hold values from -6 to 6
- step_size: float32 [12288, 2], P('seq'), may hold values from 7.564421e-05 to 0.0007564421
- gate_weight: bfloat16 [1280, 3072], P('seq', 'head'), may hold values from -1 to 1
- up_weight: bfloat16 [1280, 3072], P('seq', 'head'), may hold values from -1 to 1
- down_weight: bfloat16 [1280, 3072], P('seq', 'head'), may hold values from -1 to 1
Outputs:
- mixed: bfloat16 [12288, 2560], P('seq', 'head')
The draws below stay inside these ranges and needn't reach their ends.
All inputs are finite; a program needn't handle non-finite values.
Results may differ from the reference program's by a relative error of at most 0.0066.
Values may be sent and summed in bfloat16 or wider, within the bound.
No kernel may reach another device: no remote copies, remote signals or barrier semaphores. Data moves between devices by JAX's collectives and lax.ppermute only.
A program may use at most 128 MiB of HBM per device.

```python
import math
import jax
import jax.numpy as jnp
from jax import lax

HEADS = 2
DH = 1280
UNITS = 1536
GROUP = 12288


def fast_weight(key, salt, fan_in):
    mixed_key = jax.random.fold_in(key, salt)
    base_key, rows_key = jax.random.split(mixed_key, 2)
    column_total = HEADS * UNITS
    base = jnp.clip(jax.random.normal(base_key, (DH, column_total), jnp.float32), -6.0, 6.0)
    ramp = jnp.arange(DH, dtype=jnp.float32) / (DH - 1)
    row_scale = (10.0 ** ramp)[:, None] * jnp.exp(jax.random.uniform(rows_key, (DH, 1), jnp.float32, -0.35, 0.35))
    scaled = base * row_scale / jnp.sqrt(jnp.mean(row_scale * row_scale))
    scaled = scaled / jnp.sqrt(jnp.float32(fan_in))
    return jnp.clip(scaled, -1.0, 1.0).astype(jnp.bfloat16)


def draw_gate_weight(key, part):
    return fast_weight(key, 101, DH)


def draw_up_weight(key, part):
    return fast_weight(key, 202, DH)


def draw_down_weight(key, part):
    return fast_weight(key, 303, UNITS)


def draw_values(key, part):
    mixed_key = jax.random.fold_in(key, 404)
    noise_key, direction_key, token_key = jax.random.split(mixed_key, 3)
    width = HEADS * DH
    noise = jnp.clip(jax.random.normal(noise_key, (GROUP, width), jnp.float32), -6.0, 6.0)
    strength = 0.5
    direction = jnp.clip(jax.random.normal(direction_key, (1, width), jnp.float32), -4.0, 4.0)
    token_weight = jax.random.uniform(token_key, (GROUP, 1), jnp.float32, 0.5, 1.5)
    combined = noise + strength * token_weight * direction
    return jnp.clip(combined, -6.0, 6.0).astype(jnp.bfloat16)


def levels(key, dims, pieces, smallest, largest):
    factor_of = 1.0
    for dim, shards_of in pieces:
        draws = jax.random.uniform(jax.random.fold_in(jax.random.fold_in(key, 6), dim), (shards_of,), jnp.float32, smallest / len(pieces), largest / len(pieces))
        factor_of = factor_of * jnp.repeat(jnp.exp(draws), dims[dim] // shards_of).reshape((-1,) + (1,) * (len(dims) - 1 - dim))
    return factor_of


def centred(own_key, dims, scale, bound, shards=(), kind=jnp.bfloat16):
    gain = levels(own_key, dims, shards, -0.22, 0.18) if shards else 1.0
    values = jax.random.normal(own_key, dims, jnp.float32) * scale * gain
    return jnp.minimum(jnp.maximum(values, -bound), bound).astype(kind)


def setup_inputs(seed: int = 0) -> dict:
    arg_keys = jax.random.split(jax.random.key(seed), 8)
    return {
        "keys": centred(arg_keys[0], (GROUP, HEADS * DH), 1.0, 6.0, ((0, 8), (1, 4))),
        "values": draw_values(jax.random.fold_in(arg_keys[7], 71), 0),
        "queries": centred(arg_keys[2], (GROUP, HEADS * DH), 1.0, 6.0, ((0, 8), (1, 4))),
        "step_size": jnp.clip(jnp.exp(math.log(0.0007564421) - 2.3025851 * jax.random.uniform(arg_keys[3], (GROUP, HEADS), jnp.float32) ** levels(arg_keys[3], (GROUP, HEADS), ((0, 8),), -0.2, 0.2)), 7.564420957351103e-05, 0.0007564421),
        "gate_weight": draw_gate_weight(jax.random.fold_in(arg_keys[7], 71), 0),
        "up_weight": draw_up_weight(jax.random.fold_in(arg_keys[7], 71), 0),
        "down_weight": draw_down_weight(jax.random.fold_in(arg_keys[7], 71), 0),
    }


epsilon = 1e-06

def silu_slope(values_in):
    sigma = jax.nn.sigmoid(values_in)
    return sigma * (1.0 + values_in * (1.0 - sigma))

def norm_ratio(old_matrix, new_matrix):
    old_sums = lax.optimization_barrier(jnp.sum(jnp.square(old_matrix.astype(jnp.float32)), axis=0))
    new_sums = lax.optimization_barrier(jnp.sum(jnp.square(new_matrix.astype(jnp.float32)), axis=0))
    return jnp.sqrt((old_sums + epsilon) / (new_sums + epsilon))

def one_head(key_block, value_block, query_block, rates, weight_gate, weight_up, weight_down):
    gate_act = jnp.dot(key_block, weight_gate, preferred_element_type=jnp.float32)
    up_act = jnp.dot(key_block, weight_up, preferred_element_type=jnp.float32)
    silu_gate = jax.nn.silu(gate_act)
    hidden = (silu_gate * up_act).astype(jnp.bfloat16)
    outgrad = (-(rates * value_block.astype(jnp.float32))).astype(jnp.bfloat16)
    hidden_grad = jnp.dot(outgrad, weight_down, preferred_element_type=jnp.float32)
    gate_grad = (hidden_grad * up_act * silu_slope(gate_act)).astype(jnp.bfloat16)
    up_grad = (hidden_grad * silu_gate).astype(jnp.bfloat16)
    grad_gate = jnp.dot(key_block.T, gate_grad, preferred_element_type=jnp.float32)
    grad_up = jnp.dot(key_block.T, up_grad, preferred_element_type=jnp.float32)
    grad_down = jnp.dot(outgrad.T, hidden, preferred_element_type=jnp.float32)
    new_gate = (weight_gate.astype(jnp.float32) - grad_gate).astype(jnp.bfloat16)
    new_up = (weight_up.astype(jnp.float32) - grad_up).astype(jnp.bfloat16)
    new_down = (weight_down.astype(jnp.float32) - grad_down).astype(jnp.bfloat16)
    ratio_gate = norm_ratio(weight_gate, new_gate)
    ratio_up = norm_ratio(weight_up, new_up)
    ratio_down = norm_ratio(weight_down, new_down)
    query_gate = jnp.dot(query_block, new_gate, preferred_element_type=jnp.float32) * ratio_gate
    query_up = jnp.dot(query_block, new_up, preferred_element_type=jnp.float32) * ratio_up
    query_hidden = (jax.nn.silu(query_gate) * query_up * ratio_down).astype(jnp.bfloat16)
    return jnp.dot(query_hidden, new_down.T, preferred_element_type=jnp.float32).astype(jnp.bfloat16)

def reference(keys, values, queries, step_size, gate_weight, up_weight, down_weight):
    results = []
    for head_index in range(HEADS):
        feature_lo = head_index * DH
        unit_lo = head_index * UNITS
        results.append(one_head(keys[:, feature_lo:feature_lo + DH], values[:, feature_lo:feature_lo + DH], queries[:, feature_lo:feature_lo + DH], step_size[:, head_index:head_index + 1], gate_weight[:, unit_lo:unit_lo + UNITS], up_weight[:, unit_lo:unit_lo + UNITS], down_weight[:, unit_lo:unit_lo + UNITS]))
    return jnp.concatenate(results, axis=1)
```

```python
import jax
import jax.numpy as jnp
from jax import lax
from jax.sharding import PartitionSpec as P


epsilon = 1e-06
f32 = jnp.float32
bf16 = jnp.bfloat16
COLS = 2


def swapped(value, axis, stride):
    mask = 2**stride
    pairs = [(source, source ^ mask) for source in range(lax.axis_size(axis))]
    return lax.ppermute(value, axis, pairs)


def shifted(value, step):
    count = lax.axis_size("seq")
    pairs = [(source, (source + step * COLS) % count) for source in range(count)]
    return lax.ppermute(value, "seq", pairs)


def silu_slope(values_in):
    sigma = jax.nn.sigmoid(values_in)
    return sigma * (1.0 + values_in * (1.0 - sigma))


def square_sums(matrix):
    return jnp.sum(jnp.square(matrix.astype(f32)), axis=0)


def join_halves(own_part, other_part, half_index):
    first_half = jnp.where(half_index == 0, own_part, other_part)
    second_half = jnp.where(half_index == 0, other_part, own_part)
    return jnp.concatenate([first_half, second_half], axis=1)


def contract_rows(left, right):
    return lax.dot_general(left, right, (((0,), (0,)), ((), ())), preferred_element_type=f32)


def contract_cols(left, right):
    return lax.dot_general(left, right, (((1,), (1,)), ((), ())), preferred_element_type=f32)


def gather_rows(shard):
    rows, columns = shard.shape
    count = lax.axis_size("seq")
    if count > 8 or count % COLS:
        return lax.all_gather(shard, "seq", axis=0, tiled=True)
    lines = count // COLS
    place = lax.axis_index("seq")
    line, col = place // COLS, place % COLS
    full = jnp.zeros((lines, COLS, rows, columns), shard.dtype)
    own = [shard] + [shifted(shard, step) for step in range(1, lines)]
    other = [swapped(piece, "seq", 0) for piece in own]
    for step in range(lines):
        source = (line - step) % lines
        full = lax.dynamic_update_slice(full, own[step][None, None], (source, col, 0, 0))
        full = lax.dynamic_update_slice(full, other[step][None, None], (source, 1 - col, 0, 0))
    return full.reshape(count * rows, columns)


def scatter_rows(partial):
    count = lax.axis_size("seq")
    if count > 8 or count % COLS:
        return lax.psum_scatter(partial, "seq", scatter_dimension=0, tiled=True)
    lines = count // COLS
    place = lax.axis_index("seq")
    line, col = place // COLS, place % COLS
    rows, columns = partial.shape[0] // count, partial.shape[1]
    blocks = partial.reshape(lines, COLS, rows, columns)

    def block(step, column):
        start = ((line + step) % lines, column, 0, 0)
        return lax.dynamic_slice(blocks, start, (1, 1, rows, columns))[0, 0]

    order = list(range(1, lines)) + [0]
    got = {step: swapped(block(step, 1 - col).astype(bf16), "seq", 0) for step in order}
    pair = {step: block(step, col) + got[step].astype(f32) for step in order}
    total = pair[0]
    for step in range(1, lines):
        total = total + shifted(pair[step].astype(bf16), step).astype(f32)
    return total


def body(keys, values, queries, step_size, gate_weight, up_weight, down_weight):
    position = lax.axis_index("head")
    half_index = position % 2
    head_index = position // 2
    full_gate = gather_rows(gate_weight)
    full_up = gather_rows(up_weight)
    full_down = gather_rows(down_weight)
    other_keys, other_values, other_queries = swapped((keys, values, queries), "head", 0)
    key_full = join_halves(keys, other_keys, half_index)
    value_full = join_halves(values, other_values, half_index)
    query_full = join_halves(queries, other_queries, half_index)
    rates = lax.dynamic_slice_in_dim(step_size, head_index, 1, 1)
    outgrad = (-(rates * value_full.astype(f32))).astype(bf16)

    gate_act = jnp.dot(key_full, full_gate, preferred_element_type=f32)
    up_act = jnp.dot(key_full, full_up, preferred_element_type=f32)
    silu_gate = jax.nn.silu(gate_act)
    hidden = (silu_gate * up_act).astype(bf16)
    grad_down = scatter_rows(contract_rows(outgrad, hidden))
    hidden_grad = jnp.dot(outgrad, full_down, preferred_element_type=f32)
    gate_grad = (hidden_grad * up_act * silu_slope(gate_act)).astype(bf16)
    up_grad = (hidden_grad * silu_gate).astype(bf16)
    grad_gate = scatter_rows(contract_rows(key_full, gate_grad))
    grad_up = scatter_rows(contract_rows(key_full, up_grad))
    old_gate_sums = square_sums(full_gate)
    old_up_sums = square_sums(full_up)
    old_down_sums = square_sums(full_down)

    new_down = gather_rows((down_weight.astype(f32) - grad_down).astype(bf16))
    new_gate = gather_rows((gate_weight.astype(f32) - grad_gate).astype(bf16))
    new_up = gather_rows((up_weight.astype(f32) - grad_up).astype(bf16))
    ratio_down = jnp.sqrt((old_down_sums + epsilon) / (square_sums(new_down) + epsilon))
    ratio_gate = jnp.sqrt((old_gate_sums + epsilon) / (square_sums(new_gate) + epsilon))
    ratio_up = jnp.sqrt((old_up_sums + epsilon) / (square_sums(new_up) + epsilon))
    query_gate = jnp.dot(query_full, new_gate, preferred_element_type=f32) * ratio_gate
    query_up = jnp.dot(query_full, new_up, preferred_element_type=f32) * ratio_up
    query_hidden = (jax.nn.silu(query_gate) * query_up * ratio_down).astype(bf16)
    partial_sums = contract_cols(query_hidden, new_down)
    half_width = partial_sums.shape[1] // 2
    kept_sums = lax.dynamic_slice_in_dim(partial_sums, half_index * half_width, half_width, 1)
    sent_sums = lax.dynamic_slice_in_dim(partial_sums, (1 - half_index) * half_width, half_width, 1)
    received = swapped(sent_sums, "head", 0)
    return (kept_sums + received).astype(bf16)


def solution(mesh):
    return jax.shard_map(
        body,
        mesh=mesh,
        in_specs=(
            P("seq", "head"),
            P("seq", "head"),
            P("seq", "head"),
            P("seq", None),
            P("seq", "head"),
            P("seq", "head"),
            P("seq", "head"),
        ),
        out_specs=P("seq", "head"),
        check_vma=False,
    )
```
